8 devices in a mesh: dp: 1 (over z), tp: 8 (over x, y, core).
Axes of the slice: x: 2, y: 2, z: 1, core: 2. Of those that a mesh axis runs over, the one named last changes fastest.
Arguments:
- x: bfloat16 [2048, 5120], P('dp')
- w_gate: bfloat16 [5120, 32768], P(None, 'tp')
- w_up: bfloat16 [5120, 32768], P(None, 'tp')
- w_down: bfloat16 [32768, 5120], P('tp')
Outputs:
- output: bfloat16 [2048, 5120], P('dp')
All inputs are finite; a program needn't handle non-finite values.
Results may differ from the reference program's by a relative error of at most 0.016.
Values are sent between devices in bfloat16 or wider.
A program may use at most 2 GiB of HBM per device.

```python
import jax
import jax.numpy as jnp

ROWS = 2048
D = 5120
FF = 32768


def setup_inputs(seed: int = 0, part: int = 0) -> dict:
    kx, kg, ku, kd = jax.random.split(jax.random.key(seed), 4)
    drawn = {
        "x": jax.random.normal(jax.random.fold_in(kx, part), (ROWS, D), jnp.float32),
        "w_gate": jax.random.normal(kg, (D, FF), jnp.float32) * D**-0.5,
        "w_up": jax.random.normal(ku, (D, FF), jnp.float32) * D**-0.5,
        "w_down": jax.random.normal(kd, (FF, D), jnp.float32) * FF**-0.5,
    }
    return {k: v.astype(jnp.bfloat16) for k, v in drawn.items()}


def reference(x, w_gate, w_up, w_down):
    gate = jnp.dot(x, w_gate, preferred_element_type=jnp.float32)
    up = jnp.dot(x, w_up, preferred_element_type=jnp.float32)
    hidden = (jax.nn.silu(gate) * up).astype(jnp.bfloat16)
    return jnp.dot(hidden, w_down, preferred_element_type=jnp.float32).astype(jnp.bfloat16)
```

```python
import functools

import jax
import jax.numpy as jnp
from jax import lax
from jax.experimental import pallas as pl
from jax.experimental.pallas import tpu as pltpu
from jax.sharding import PartitionSpec as P

MESH = pl.DeviceIdType.MESH
CHUNKS = (512, 512, 512, 512)
TF = 256
TD = 512
SLOTS = 3
AHEAD = SLOTS - 1
F32, BF16 = jnp.float32, jnp.bfloat16

STRIDE = 2
LAGS = (1, 3, 5, 7, 9, 11)
COMM = True


def al(i, m=16):
    return pl.multiple_of(i, m)


def kernel(x_hbm, wg_hbm, wu_hbm, wd_hbm, y_hbm, xbuf, h, w, own, send_a, recv_a, send_b, recv_b,
           send_c, recv_c, fin, wsem, xsem, ssem, rsem):
    depth, ff = wg_hbm.shape
    n_g, n_d = ff // TF, depth // TD
    period = n_g + n_d

    tp = lax.axis_index("tp")
    core = tp % 2
    yb = (tp // 2) % 2
    xb = tp // 4
    partner = tp + 1 - 2 * core
    xn = tp + 4 - 8 * xb
    yn = tp + 2 - 4 * yb
    n1 = xn + core * (yn - xn)
    n2 = yn + core * (xn - yn)
    p1 = xb + core * (yb - xb)
    p2 = yb + core * (xb - yb)

    if COMM:
        barrier = pltpu.get_barrier_semaphore()
        for dev in (partner, xn, yn):
            pl.semaphore_signal(barrier, inc=1, device_id={"tp": dev}, device_id_type=MESH)
        pl.semaphore_wait(barrier, 3)

    def weights(slot, t, gate_up):
        if gate_up:
            cols = pl.ds(al(t * TF, TF), TF)
            return (pltpu.make_async_copy(wg_hbm.at[:, cols], w.at[slot, :, pl.ds(0, TF)], wsem.at[slot, 0]),
                    pltpu.make_async_copy(wu_hbm.at[:, cols], w.at[slot, :, pl.ds(TF, TF)], wsem.at[slot, 1]))
        cols = pl.ds(al(t * TD, TD), TD)
        return (pltpu.make_async_copy(wd_hbm.at[:, cols], w.at[slot, pl.ds(0, ff), pl.ds(0, TD)], wsem.at[slot, 0]),)

    def issue(slot, t, gate_up):
        for copy in weights(slot, t, gate_up):
            copy.start()

    def x_copy(r0, rows):
        return pltpu.make_async_copy(x_hbm.at[pl.ds(r0, rows)], xbuf.at[pl.ds(0, rows)], xsem)

    def remote(src, dst, j, s, r, dev):
        return pltpu.make_async_remote_copy(
            src_ref=src, dst_ref=dst, send_sem=ssem.at[j, s], recv_sem=rsem.at[j, r],
            device_id={"tp": dev}, device_id_type=MESH)

    def copies(r0, rows, j):
        half, quarter, eighth = rows // 2, rows // 4, rows // 8
        cols = pl.ds(al(j * TD, TD), TD)

        def y_at(off, n):
            return y_hbm.at[pl.ds(al(off), n), cols]

        mine = r0 + core * half
        theirs = r0 + (1 - core) * half
        piece = y_at(mine + p1 * quarter + p2 * eighth, eighth)
        piece2 = y_at(mine + p1 * quarter + (1 - p2) * eighth, eighth)
        piece1 = y_at(mine + (1 - p1) * quarter + p2 * eighth, eighth)
        piece12 = y_at(mine + (1 - p1) * quarter + (1 - p2) * eighth, eighth)
        quarter1 = y_at(mine + (1 - p1) * quarter, quarter)
        their = y_at(theirs + p2 * quarter + p1 * eighth, eighth)
        their2 = y_at(theirs + p2 * quarter + (1 - p1) * eighth, eighth)
        theirq = y_at(theirs + (1 - p2) * quarter, quarter)
        f = fin.at[j, pl.ds(0, eighth)]
        sa, ra = send_a.at[j, pl.ds(0, half)], recv_a.at[j, pl.ds(0, half)]
        sb, rb = send_b.at[j, pl.ds(0, quarter)], recv_b.at[j, pl.ds(0, quarter)]
        sc, rc = send_c.at[j, pl.ds(0, eighth)], recv_c.at[j, pl.ds(0, eighth)]
        out = dict(
            a=lambda: remote(sa, ra, j, 0, 0, partner),
            b=lambda: remote(sb, rb, j, 1, 1, n1),
            c=lambda: remote(sc, rc, j, 2, 2, n2),
            local=lambda: pltpu.make_async_copy(f, piece, ssem.at[j, 3]),
            f2=lambda: remote(f, piece, j, 4, 3, n2),
            f1=lambda: remote(f, piece, j, 5, 4, n1),
            fp=lambda: remote(f, piece, j, 6, 6, partner),
            g1=lambda: remote(piece2, piece2, j, 7, 5, n1),
            gp=lambda: remote(piece2, piece2, j, 8, 7, partner),
            qp=lambda: remote(quarter1, quarter1, j, 9, 8, partner),
        )
        waits = dict(
            f2=lambda: remote(f, piece2, j, 4, 3, n2),
            f1=lambda: remote(f, piece1, j, 5, 4, n1),
            g1=lambda: remote(piece2, piece12, j, 7, 5, n1),
            fp=lambda: remote(f, their, j, 6, 6, partner),
            gp=lambda: remote(piece2, their2, j, 8, 7, partner),
            qp=lambda: remote(quarter1, theirq, j, 9, 8, partner),
        )
        return out, waits

    def stage_b(r0, rows, j):
        half, quarter, eighth = rows // 2, rows // 4, rows // 8
        c, _ = copies(r0, rows, j)
        c["a"]().wait_recv()
        go = pl.ds(al((1 - p1) * quarter), quarter)
        keep = pl.ds(al(p1 * quarter), quarter)
        send_b[j, pl.ds(0, quarter)] = (own[j, go] + recv_a[j, go].astype(F32)).astype(BF16)
        c["b"]().start()
        own[j, keep] = own[j, keep] + recv_a[j, keep].astype(F32)

    def stage_c(r0, rows, j):
        half, quarter, eighth = rows // 2, rows // 4, rows // 8
        c, _ = copies(r0, rows, j)
        c["b"]().wait_recv()
        go = pl.ds(al(p1 * quarter + (1 - p2) * eighth), eighth)
        keep = pl.ds(al(p1 * quarter + p2 * eighth), eighth)
        send_c[j, pl.ds(0, eighth)] = (
            own[j, go] + recv_b[j, pl.ds(al((1 - p2) * eighth), eighth)].astype(F32)).astype(BF16)
        c["c"]().start()
        own[j, keep] = own[j, keep] + recv_b[j, pl.ds(al(p2 * eighth), eighth)].astype(F32)

    def stage_f(r0, rows, j):
        half, quarter, eighth = rows // 2, rows // 4, rows // 8
        c, _ = copies(r0, rows, j)
        c["c"]().wait_recv()
        keep = pl.ds(al(p1 * quarter + p2 * eighth), eighth)
        fin[j, pl.ds(0, eighth)] = (own[j, keep] + recv_c[j, pl.ds(0, eighth)].astype(F32)).astype(BF16)
        c["f2"]().start()
        c["f1"]().start()
        c["fp"]().start()
        c["local"]().start()

    def stage_g(r0, rows, j):
        c, got = copies(r0, rows, j)
        got["f2"]().wait_recv()
        c["g1"]().start()
        c["gp"]().start()

    def stage_q(r0, rows, j):
        c, got = copies(r0, rows, j)
        got["f1"]().wait_recv()
        got["g1"]().wait_recv()
        c["qp"]().start()

    def stage_e(r0, rows, j):
        c, got = copies(r0, rows, j)
        for k in ("fp", "gp", "qp"):
            got[k]().wait_recv()
        c["local"]().wait()
        for k in ("a", "b", "c", "f2", "f1", "fp", "g1", "gp", "qp"):
            c[k]().wait_send()

    stages = (stage_b, stage_c, stage_f, stage_g, stage_q, stage_e)

    def tick(r0, rows, t, stride, lo=0):
        if not COMM:
            return
        for lag, stage in zip(LAGS, stages):
            u = t - lag
            j = (u + 64 * stride) // stride - 64
            due = (u >= 0) & (u < stride * n_d) & ((u + 64 * stride) % stride == 0)
            pl.when(due)(functools.partial(stage, r0, rows, j))

    n_ticks = lambda stride: LAGS[-1] + stride * (n_d - 1) + 1

    r0s = [sum(CHUNKS[:i]) for i in range(len(CHUNKS))]
    x_copy(r0s[0], CHUNKS[0]).start()
    for t in range(AHEAD):
        issue(t % SLOTS, t, True)

    for c, (r0, rows) in enumerate(zip(r0s, CHUNKS)):
        half = rows // 2
        base = c * period
        x_copy(r0, rows).wait()

        def gate_up_step(s, _, c=c, base=base, rows=rows):
            slot = (base + s) % SLOTS
            nslot = (base + s + AHEAD) % SLOTS
            nxt = s + AHEAD
            pl.when(nxt < n_g)(lambda: issue(nslot, nxt, True))
            pl.when(nxt >= n_g)(lambda: issue(nslot, nxt - n_g, False))
            if c > 0:
                tick(r0s[c - 1], CHUNKS[c - 1], n_d + s, STRIDE)
            for copy in weights(slot, s, True):
                copy.wait()
            r = jnp.dot(xbuf[pl.ds(0, rows)], w[slot], preferred_element_type=F32)
            gate, up = r[:, :TF], r[:, TF:]
            h[pl.ds(0, rows), pl.ds(al(s * TF, TF), TF)] = (gate / (1.0 + jnp.exp(-gate)) * up).astype(BF16)
            return 0

        lax.fori_loop(0, n_g, gate_up_step, 0)
        last = c == len(CHUNKS) - 1
        if not last:
            x_copy(r0s[c + 1], CHUNKS[c + 1]).start()

        def down_step(j, _, c=c, base=base, rows=rows, r0=r0, last=last):
            half = rows // 2
            slot = (base + n_g + j) % SLOTS
            nslot = (base + n_g + j + AHEAD) % SLOTS
            nxt = j + AHEAD
            pl.when(nxt < n_d)(lambda: issue(nslot, nxt, False))
            if not last:
                pl.when(nxt >= n_d)(lambda: issue(nslot, nxt - n_d, True))
            if c > 0:
                tick(r0s[c - 1], CHUNKS[c - 1], n_d + n_g + j, STRIDE)
            tick(r0, rows, j, 1 if last else STRIDE)
            for copy in weights(slot, j, False):
                copy.wait()
            wd = w[slot, pl.ds(0, ff), pl.ds(0, TD)]
            send_a[j, pl.ds(0, half)] = jnp.dot(
                h[pl.ds(al((1 - core) * half), half)], wd, preferred_element_type=F32).astype(BF16)
            if COMM:
                copies(r0, rows, j)[0]["a"]().start()
            own[j, pl.ds(0, half)] = jnp.dot(
                h[pl.ds(al(core * half), half)], wd, preferred_element_type=F32)
            return 0

        lax.fori_loop(0, n_d, down_step, 0)

    def tail(t, _):
        tick(r0s[-1], CHUNKS[-1], t, 1)
        return 0

    if COMM:
        lax.fori_loop(n_d, n_ticks(1), tail, 0)


def solution(mesh):
    def step(x, w_gate, w_up, w_down):
        depth, ff = w_gate.shape
        n_d = depth // TD
        rows = max(CHUNKS)
        hbm = pl.BlockSpec(memory_space=pl.ANY)
        y = pl.pallas_call(
            kernel,
            out_shape=jax.ShapeDtypeStruct(x.shape, x.dtype),
            in_specs=[hbm] * 4,
            out_specs=hbm,
            scratch_shapes=[
                pltpu.VMEM((rows, depth), BF16),
                pltpu.VMEM((rows, ff), BF16),
                pltpu.VMEM((SLOTS, depth, max(2 * TF, TD)), BF16),
                pltpu.VMEM((n_d, rows // 2, TD), F32),
                pltpu.VMEM((n_d, rows // 2, TD), BF16),
                pltpu.VMEM((n_d, rows // 2, TD), BF16),
                pltpu.VMEM((n_d, rows // 4, TD), BF16),
                pltpu.VMEM((n_d, rows // 4, TD), BF16),
                pltpu.VMEM((n_d, rows // 8, TD), BF16),
                pltpu.VMEM((n_d, rows // 8, TD), BF16),
                pltpu.VMEM((n_d, rows // 8, TD), BF16),
                pltpu.SemaphoreType.DMA((SLOTS, 2)),
                pltpu.SemaphoreType.DMA,
                pltpu.SemaphoreType.DMA((n_d, 10)),
                pltpu.SemaphoreType.DMA((n_d, 9)),
            ],
            compiler_params=pltpu.CompilerParams(
                collective_id=0 if COMM else None, has_side_effects=True, vmem_limit_bytes=60 * 2**20),
            name="mlp",
        )(x, w_gate, w_up, w_down)
        return y

    return jax.shard_map(
        step,
        mesh=mesh,
        in_specs=(P("dp", None), P(None, "tp"), P(None, "tp"), P("tp", None)),
        out_specs=P("dp", None),
        check_vma=False,
    )
```
